256 devices in a mesh: group: 2 (over y), pool: 2 (over core), slab: 64 (over z, x).
Axes of the slice: x: 4, y: 2, z: 16, core: 2. Of those that a mesh axis runs over, the one named last changes fastest.
The devices are a block of a 4x16x16 slice.
Arguments:
- drho_part: float32 [2, 32, 2, 128, 128, 128], P('pool', 'group', None, 'slab'), parts along dimension 1, may hold values from -6 to 6
- fxc: float32 [128, 128, 128], P('slab'), may hold values from -2 to -0.2
- cutoff_mask: int32 [128, 128, 128], P(None, 'slab'), may hold values 0 or 1
- owner_table: int32 [32], P('group'), parts along dimension 0, may hold values from 0 to 15, each once
Outputs:
- dv: float32 [32, 2, 128, 128, 128], P('group', None, 'slab'), parts along dimension 0
The draws below stay inside these ranges and needn't reach their ends.
There are 2 independent parts, one for each index of `group`. The reference program is written for one: setup_inputs(seed, part) draws one part's arguments, and reference() takes and returns one part's arrays. A program takes and returns all parts, laid end to end along the dimension named above; an argument that names none is the same for every part. Nothing has to cross between parts.
Inputs may be any that keep to these rules, and one draw needn't show every extreme that they name: `owner_table`: each perturbation appears in exactly one slot.
All inputs are finite; a program needn't handle non-finite values. No bound on the sum of `cutoff_mask` on one device may be relied on, other than what follows from the above.
Results may differ from the reference program's by a relative error of at most 0.00008.
Values sent between devices are 32-bit elements; how exact they have to be, the bound alone decides.
A program may use at most 64 MiB of HBM per device.

```python
import math
import jax
import jax.numpy as jnp
from jax import lax

NG = 128
P_SIZE = 16
N_POOL = 2


def set_ends(array, rng, smallest, top_value):
    longest = array.shape.index(max(array.shape))
    spots = []
    for shift in (0, 1):
        where = [jax.random.randint(jax.random.fold_in(rng, axis), (), 0, length) for axis, length in enumerate(array.shape)]
        where[longest] = (where[longest] + shift) % array.shape[longest]
        spots.append(tuple(where))
    return array.at[spots[0]].set(smallest).at[spots[1]].set(top_value)


def shard_levels(stream_key, extent, cuts, low, top_value):
    level, own = 1.0, jax.random.fold_in(stream_key, 6)
    for position, shards_of in cuts:
        steps = jnp.exp(jax.random.uniform(jax.random.fold_in(own, position), (shards_of,), jnp.float32, low / len(cuts), top_value / len(cuts)))
        level = level * jnp.repeat(steps, extent[position] // shards_of).reshape([-1 if axis == position else 1 for axis in range(len(extent))])
    return level


def gaussian(stream_key, extent, width, reach, pieces=(), kind=jnp.bfloat16):
    drawn = jax.random.normal(stream_key, extent, jnp.float32) * width
    if len(pieces) > 0:
        drawn = shard_levels(stream_key, extent, pieces, -0.22, 0.18) * drawn
    return jnp.clip(drawn, min=-reach, max=reach).astype(kind)


def setup_inputs(seed: int = 0, part: int = 0) -> dict:
    key_of = jax.random.split(jax.random.key(seed), 5)
    own_keys = jax.random.split(jax.random.fold_in(key_of[4], part), 5)
    drho_part = gaussian(own_keys[0], (N_POOL, P_SIZE, 2, NG, NG, NG), 1.0, 6.0, ((0, 2), (3, 64)), jnp.float32)
    fxc = jnp.clip(-2.0 + 1.8 * jax.random.uniform(key_of[1], (NG, NG, NG), jnp.float32) ** shard_levels(key_of[1], (NG, NG, NG), ((0, 64),), -0.2, 0.2), -2.0, -0.2)
    cutoff_mask = set_ends((jax.random.randint(key_of[2], (NG, NG, NG), 0, 4) < 3).astype(jnp.int32), jax.random.fold_in(key_of[2], 1), 0, 1)
    owner_table = jax.random.permutation(own_keys[3], P_SIZE).astype(jnp.int32)
    return dict(drho_part=drho_part, fxc=fxc, cutoff_mask=cutoff_mask, owner_table=owner_table)


def kernel_table(cutoff_mask):
    index = jnp.arange(NG, dtype=jnp.int32)
    freq = ((index + NG // 2) % NG - NG // 2).astype(jnp.float32)
    square = freq * freq
    total = square[:, None, None] + square[None, :, None] + square[None, None, :]
    unit = (2.0 * math.pi / NG) ** 2
    return 4.0 * math.pi * cutoff_mask.astype(jnp.float32) / (unit * total + 0.25)


def reference(drho_part, fxc, cutoff_mask, owner_table):
    density = jnp.sum(drho_part, axis=0)
    ordered = jnp.take(density, owner_table, axis=0)
    kernel = kernel_table(cutoff_mask)

    def single(field):
        spectrum = jnp.fft.fftn(lax.complex(field[0], field[1]))
        hartree = jnp.fft.ifftn(spectrum * kernel)
        return jnp.stack([jnp.real(hartree) + fxc * field[0], jnp.imag(hartree) + fxc * field[1]])

    return lax.map(single, ordered)
```

```python
import functools
import math

import jax
import jax.numpy as jnp
import numpy as np
from jax import lax
from jax.experimental import pallas as pl
from jax.experimental.pallas import tpu as pltpu
from jax.sharding import PartitionSpec as P

MESH = pl.DeviceIdType.MESH


def complex_form(table):
    return np.block([[table.real, -table.imag], [table.imag, table.real]])


def two_halves(table):
    high = table.astype(np.float32).astype(jnp.bfloat16)
    low = (table - high.astype(np.float64)).astype(np.float32).astype(jnp.bfloat16)
    return np.stack([high, low])


def dft_tables(length, width):
    tiles = length // width
    index = np.arange(length)
    phase = np.exp(-2j * math.pi * (index[:, None] * index[None, :] % length) / length)
    lanes = complex_form(phase).T
    real = complex_form(phase).reshape(2, length, 2, length)
    same = np.eye(width)
    cut = real.reshape(2, tiles, width, 2, length)
    spread = np.einsum("atibn,mk->tamibkn", cut, same)
    spread = spread.reshape(tiles * 2 * width * width, 2 * width * length)
    cut = real.reshape(2, length, 2, tiles, width)
    gather = np.einsum("anbtm,ik->aintbmk", cut, same)
    gather = gather.reshape(2 * width * length, tiles * 2 * width * width)
    return two_halves(lanes), two_halves(spread), two_halves(gather)


def split(value):
    high = value.astype(jnp.bfloat16)
    low = (value - high.astype(jnp.float32)).astype(jnp.bfloat16)
    return high, low


def from_left(table, value):
    high, low = split(value)
    lanes = value.shape[1]
    both = jnp.concatenate([high, low], axis=1)
    most = jnp.dot(table[0], both, preferred_element_type=jnp.float32)
    rest = jnp.dot(table[1], high, preferred_element_type=jnp.float32)
    return most[:, :lanes] + (most[:, lanes:] + rest)


def along_lanes(table, value):
    high, low = split(value)
    rows = value.shape[0]
    both = jnp.concatenate([high, low], axis=0)
    most = jnp.dot(both, table[0], preferred_element_type=jnp.float32)
    rest = jnp.dot(high, table[1], preferred_element_type=jnp.float32)
    return most[:rows] + (most[rows:] + rest)


def frequency(index, length):
    return ((index + length // 2) % length - length // 2).astype(jnp.float32)


def body(
    slabs, pools, owner_ref, drho_hbm, fxc_hbm, mask_hbm, lanes_hbm, spread_hbm, gather_hbm, out_hbm,
    drho, fxc, mask, lanes, spread, gather, kernel, other, given, density, sent, columns, back, final, result,
    load_sem, other_sem, send_sem, column_sem, final_sem, out_sem,
):
    me = lax.axis_index("slab")
    pool = lax.axis_index("pool")
    partner = pools - 1 - pool
    owned = given.shape[0]
    rows, length = given.shape[1:]
    half = rows // 2
    width = mask.shape[1]

    loads = [
        pltpu.make_async_copy(source, target, load_sem.at[n])
        for n, (source, target) in enumerate(
            [
                (drho_hbm, drho),
                (lanes_hbm, lanes),
                (spread_hbm, spread),
                (gather_hbm, gather),
                (mask_hbm, mask),
                (fxc_hbm, fxc),
            ]
        )
    ]
    for load in loads:
        load.start()

    barrier = pltpu.get_barrier_semaphore()

    def greet(step, _):
        pl.semaphore_signal(
            barrier, inc=1, device_id={"slab": lax.rem(me + step, slabs)}, device_id_type=MESH
        )
        return 0

    lax.fori_loop(1, slabs, greet, 0)
    pl.semaphore_signal(barrier, inc=1, device_id={"pool": partner}, device_id_type=MESH)

    loads[0].wait()

    def pick(slot, _):
        other[slot] = drho[owner_ref[partner * owned + slot]]
        return 0

    lax.fori_loop(0, owned, pick, 0)
    pl.semaphore_wait(barrier, slabs)

    def to_partner(slot):
        return pltpu.make_async_remote_copy(
            src_ref=other.at[slot],
            dst_ref=given.at[slot],
            send_sem=send_sem.at[0],
            recv_sem=other_sem.at[slot],
            device_id={"pool": partner},
            device_id_type=MESH,
        )

    def hand_over(slot, _):
        to_partner(slot).start()
        return 0

    lax.fori_loop(0, owned, hand_over, 0)

    def scatter(source, target, slot, arrived, left):
        def send(step, _):
            to = lax.rem(me + step, slabs)
            pltpu.make_async_remote_copy(
                src_ref=source.at[slot, to],
                dst_ref=target.at[slot, me],
                send_sem=left,
                recv_sem=arrived.at[slot],
                device_id={"slab": to},
                device_id_type=MESH,
            ).start()
            return 0

        lax.fori_loop(1, slabs, send, 0)
        target[slot, me] = source[slot, me]

    def await_all(target, slot, arrived):
        block = target.at[slot, pl.ds(0, slabs - 1)]
        pltpu.make_async_copy(block, block, arrived.at[slot]).wait()

    def await_sent(source, left):
        block = source.at[:, pl.ds(0, slabs - 1)]
        pltpu.make_async_copy(block, block, left).wait()

    loads[1].wait()
    loads[2].wait()

    def forward(slot, _):
        to_partner(slot).wait_recv()
        value = drho[owner_ref[pool * owned + slot]] + given[slot]
        density[slot] = value
        value = along_lanes(lanes, jnp.concatenate([value[:half], value[half:]], axis=1))
        value = from_left(spread, jnp.concatenate([value[:, :length], value[:, length:]], axis=0))
        sent[slot] = value.reshape(sent.shape[1:])
        scatter(sent, columns, slot, column_sem, send_sem.at[1])
        return 0

    lax.fori_loop(0, owned, forward, 0)

    for load in loads[3:]:
        load.wait()
    unit = (2.0 * math.pi / length) ** 2
    shape = (length, length)
    first = frequency(lax.broadcasted_iota(jnp.int32, shape, 0), length) ** 2
    last = frequency(lax.broadcasted_iota(jnp.int32, shape, 1), length) ** 2
    for part in range(width):
        middle = frequency(jnp.full(shape, me * width + part, jnp.int32), length) ** 2
        total = first + middle + last
        kept = mask[:, part, :].astype(jnp.float32)
        kernel[pl.ds(part * length, length)] = (
            4.0 * math.pi * kept / (unit * total + 0.25) * (1.0 / length**3)
        )

    def screen(slot, _):
        await_all(columns, slot, column_sem)
        value = from_left(gather, columns[slot].reshape(rows, length))
        factor = kernel[...]
        value = jnp.concatenate([value[:half] * factor, value[half:] * -factor], axis=0)
        back[slot] = from_left(spread, value).reshape(back.shape[1:])
        scatter(back, final, slot, final_sem, send_sem.at[2])
        return 0

    lax.fori_loop(0, owned, screen, 0)

    def outgoing(slot):
        place = out_hbm.at[pool * owned + slot]
        keep = pltpu.make_async_copy(result.at[slot], place, out_sem.at[0])
        give = pltpu.make_async_remote_copy(
            src_ref=result.at[slot],
            dst_ref=place,
            send_sem=out_sem.at[1],
            recv_sem=out_sem.at[2],
            device_id={"pool": partner},
            device_id_type=MESH,
        )
        return keep, give

    def inverse(slot, _):
        await_all(final, slot, final_sem)
        value = from_left(gather, final[slot].reshape(rows, length))
        value = along_lanes(lanes, jnp.concatenate([value[:half], value[half:]], axis=1))
        local = fxc[...]
        result[slot, pl.ds(0, half)] = value[:, :length] + local * density[slot, pl.ds(0, half)]
        result[slot, pl.ds(half, half)] = local * density[slot, pl.ds(half, half)] - value[:, length:]
        keep, give = outgoing(slot)
        keep.start()
        give.start()
        return 0

    lax.fori_loop(0, owned, inverse, 0)

    pltpu.make_async_copy(other, other, send_sem.at[0]).wait()
    await_sent(sent, send_sem.at[1])
    await_sent(back, send_sem.at[2])
    for n in range(3):
        pltpu.make_async_copy(result, result, out_sem.at[n]).wait()


def per_device(slabs, pools, drho_part, fxc, cutoff_mask, owner_table):
    _, slots, parts, planes, length, _ = drho_part.shape
    rows = parts * planes * length
    owned = slots // pools
    tables = dft_tables(length, planes)
    tile = parts * planes * planes
    field = (owned, rows, length)
    cut = (owned, slabs, tile, length)
    bf16, f32 = jnp.bfloat16, jnp.float32
    anywhere = pl.BlockSpec(memory_space=pl.ANY)
    out = pl.pallas_call(
        functools.partial(body, slabs, pools),
        out_shape=jax.ShapeDtypeStruct((slots, rows, length), f32),
        in_specs=[pl.BlockSpec(memory_space=pltpu.SMEM)] + [anywhere] * 6,
        out_specs=anywhere,
        scratch_shapes=[
            pltpu.VMEM((slots, rows, length), f32),
            pltpu.VMEM((planes * length, length), f32),
            pltpu.VMEM(cutoff_mask.shape, jnp.int32),
            *[pltpu.VMEM(table.shape, bf16) for table in tables],
            pltpu.VMEM((planes * length, length), f32),
            *[pltpu.VMEM(field, f32)] * 3,
            *[pltpu.VMEM(cut, f32)] * 4,
            pltpu.VMEM(field, f32),
            pltpu.SemaphoreType.DMA((6,)),
            pltpu.SemaphoreType.DMA((owned,)),
            pltpu.SemaphoreType.DMA((3,)),
            pltpu.SemaphoreType.DMA((owned,)),
            pltpu.SemaphoreType.DMA((owned,)),
            pltpu.SemaphoreType.DMA((3,)),
        ],
        compiler_params=pltpu.CompilerParams(
            collective_id=0, has_side_effects=True, vmem_limit_bytes=44 * 2**20
        ),
        name="response",
    )(
        owner_table,
        drho_part.reshape(slots, rows, length),
        fxc.reshape(planes * length, length),
        cutoff_mask,
        *[jnp.asarray(table) for table in tables],
    )
    return out.reshape(slots, parts, planes, length, length)


def solution(mesh):
    placed = (
        P("pool", "group", None, "slab", None, None),
        P("slab", None, None),
        P(None, "slab", None),
        P("group"),
    )
    return jax.shard_map(
        functools.partial(per_device, mesh.shape["slab"], mesh.shape["pool"]),
        mesh=mesh,
        in_specs=placed,
        out_specs=P("group", None, "slab", None, None),
        check_vma=False,
    )
```

```python
import functools
import math

import jax
import jax.numpy as jnp
import numpy as np
from jax import lax
from jax.experimental import pallas as pl
from jax.experimental.pallas import tpu as pltpu
from jax.sharding import PartitionSpec as P

MESH = pl.DeviceIdType.MESH


def complex_form(table):
    return np.block([[table.real, -table.imag], [table.imag, table.real]])


def two_halves(table):
    high = table.astype(np.float32).astype(jnp.bfloat16)
    low = (table - high.astype(np.float64)).astype(np.float32).astype(jnp.bfloat16)
    return np.stack([high, low])


def dft_tables(length, width):
    tiles = length // width
    index = np.arange(length)
    phase = np.exp(-2j * math.pi * (index[:, None] * index[None, :] % length) / length)
    lanes = complex_form(phase).T
    real = complex_form(phase).reshape(2, length, 2, length)
    same = np.eye(width)
    cut = real.reshape(2, tiles, width, 2, length)
    spread = np.einsum("atibn,mk->tamibkn", cut, same)
    spread = spread.reshape(tiles * 2 * width * width, 2 * width * length)
    cut = real.reshape(2, length, 2, tiles, width)
    gather = np.einsum("anbtm,ik->aintbmk", cut, same)
    gather = gather.reshape(2 * width * length, tiles * 2 * width * width)
    return two_halves(lanes), two_halves(spread), two_halves(gather)


def split(value):
    high = value.astype(jnp.bfloat16)
    low = (value - high.astype(jnp.float32)).astype(jnp.bfloat16)
    return high, low


def from_left(table, value):
    high, low = split(value)
    lanes = value.shape[1]
    both = jnp.concatenate([high, low], axis=1)
    most = jnp.dot(table[0], both, preferred_element_type=jnp.float32)
    rest = jnp.dot(table[1], high, preferred_element_type=jnp.float32)
    return most[:, :lanes] + (most[:, lanes:] + rest)


def along_lanes(table, value):
    high, low = split(value)
    rows = value.shape[0]
    both = jnp.concatenate([high, low], axis=0)
    most = jnp.dot(both, table[0], preferred_element_type=jnp.float32)
    rest = jnp.dot(high, table[1], preferred_element_type=jnp.float32)
    return most[:rows] + (most[rows:] + rest)


def frequency(index, length):
    return ((index + length // 2) % length - length // 2).astype(jnp.float32)


def body(
    slabs, pools, owner_hbm, drho_hbm, fxc_hbm, mask_hbm, lanes_hbm, spread_hbm, gather_hbm, out_hbm,
    owner_ref, drho, fxc, mask, lanes, spread, gather, kernel, other, given, density, sent, columns, back, final, result,
    load_sem, other_sem, send_sem, column_sem, final_sem, out_sem,
):
    me = lax.axis_index("slab")
    pool = lax.axis_index("pool")
    partner = pools - 1 - pool
    owned = given.shape[0]
    rows, length = given.shape[1:]
    half = rows // 2
    width = mask.shape[1]

    loads = [
        pltpu.make_async_copy(source, target, load_sem.at[n])
        for n, (source, target) in enumerate(
            [
                (owner_hbm, owner_ref),
                (drho_hbm, drho),
                (lanes_hbm, lanes),
                (spread_hbm, spread),
                (gather_hbm, gather),
                (mask_hbm, mask),
                (fxc_hbm, fxc),
            ]
        )
    ]
    for load in loads:
        load.start()

    barrier = pltpu.get_barrier_semaphore()

    def greet(step, _):
        pl.semaphore_signal(
            barrier, inc=1, device_id={"slab": lax.rem(me + step, slabs)}, device_id_type=MESH
        )
        return 0

    lax.fori_loop(1, slabs, greet, 0)
    pl.semaphore_signal(barrier, inc=1, device_id={"pool": partner}, device_id_type=MESH)

    loads[0].wait()
    loads[1].wait()

    def pick(slot, _):
        other[slot] = drho[owner_ref[partner * owned + slot]]
        return 0

    lax.fori_loop(0, owned, pick, 0)
    pl.semaphore_wait(barrier, slabs)

    def to_partner(slot):
        return pltpu.make_async_remote_copy(
            src_ref=other.at[slot],
            dst_ref=given.at[slot],
            send_sem=send_sem.at[0],
            recv_sem=other_sem.at[slot],
            device_id={"pool": partner},
            device_id_type=MESH,
        )

    def hand_over(slot, _):
        to_partner(slot).start()
        return 0

    lax.fori_loop(0, owned, hand_over, 0)

    def scatter(source, target, slot, arrived, left):
        def send(step, _):
            to = lax.rem(me + step, slabs)
            pltpu.make_async_remote_copy(
                src_ref=source.at[slot, to],
                dst_ref=target.at[slot, me],
                send_sem=left,
                recv_sem=arrived.at[slot],
                device_id={"slab": to},
                device_id_type=MESH,
            ).start()
            return 0

        lax.fori_loop(1, slabs, send, 0)
        target[slot, me] = source[slot, me]

    def await_all(target, slot, arrived):
        block = target.at[slot, pl.ds(0, slabs - 1)]
        pltpu.make_async_copy(block, block, arrived.at[slot]).wait()

    def await_sent(source, left):
        block = source.at[:, pl.ds(0, slabs - 1)]
        pltpu.make_async_copy(block, block, left).wait()

    loads[2].wait()
    loads[3].wait()

    def forward(slot, _):
        to_partner(slot).wait_recv()
        value = drho[owner_ref[pool * owned + slot]] + given[slot]
        density[slot] = value
        value = along_lanes(lanes, jnp.concatenate([value[:half], value[half:]], axis=1))
        value = from_left(spread, jnp.concatenate([value[:, :length], value[:, length:]], axis=0))
        sent[slot] = value.reshape(sent.shape[1:])
        scatter(sent, columns, slot, column_sem, send_sem.at[1])
        return 0

    lax.fori_loop(0, owned, forward, 0)

    for load in loads[4:]:
        load.wait()
    unit = (2.0 * math.pi / length) ** 2
    shape = (length, length)
    first = frequency(lax.broadcasted_iota(jnp.int32, shape, 0), length) ** 2
    last = frequency(lax.broadcasted_iota(jnp.int32, shape, 1), length) ** 2
    for part in range(width):
        middle = frequency(jnp.full(shape, me * width + part, jnp.int32), length) ** 2
        total = first + middle + last
        kept = mask[:, part, :].astype(jnp.float32)
        kernel[pl.ds(part * length, length)] = (
            4.0 * math.pi * kept / (unit * total + 0.25) * (1.0 / length**3)
        )

    def screen(slot, _):
        await_all(columns, slot, column_sem)
        value = from_left(gather, columns[slot].reshape(rows, length))
        factor = kernel[...]
        value = jnp.concatenate([value[:half] * factor, value[half:] * -factor], axis=0)
        back[slot] = from_left(spread, value).reshape(back.shape[1:])
        scatter(back, final, slot, final_sem, send_sem.at[2])
        return 0

    lax.fori_loop(0, owned, screen, 0)

    def outgoing(slot):
        place = out_hbm.at[pool * owned + slot]
        keep = pltpu.make_async_copy(result.at[slot], place, out_sem.at[0])
        give = pltpu.make_async_remote_copy(
            src_ref=result.at[slot],
            dst_ref=place,
            send_sem=out_sem.at[1],
            recv_sem=out_sem.at[2],
            device_id={"pool": partner},
            device_id_type=MESH,
        )
        return keep, give

    def inverse(slot, _):
        await_all(final, slot, final_sem)
        value = from_left(gather, final[slot].reshape(rows, length))
        value = along_lanes(lanes, jnp.concatenate([value[:half], value[half:]], axis=1))
        local = fxc[...]
        result[slot, pl.ds(0, half)] = value[:, :length] + local * density[slot, pl.ds(0, half)]
        result[slot, pl.ds(half, half)] = local * density[slot, pl.ds(half, half)] - value[:, length:]
        keep, give = outgoing(slot)
        keep.start()
        give.start()
        return 0

    lax.fori_loop(0, owned, inverse, 0)

    pltpu.make_async_copy(other, other, send_sem.at[0]).wait()
    await_sent(sent, send_sem.at[1])
    await_sent(back, send_sem.at[2])
    for n in range(3):
        pltpu.make_async_copy(result, result, out_sem.at[n]).wait()


def per_device(slabs, pools, drho_part, fxc, cutoff_mask, owner_table):
    _, slots, parts, planes, length, _ = drho_part.shape
    rows = parts * planes * length
    owned = slots // pools
    tables = dft_tables(length, planes)
    tile = parts * planes * planes
    field = (owned, rows, length)
    cut = (owned, slabs, tile, length)
    bf16, f32 = jnp.bfloat16, jnp.float32
    anywhere = pl.BlockSpec(memory_space=pl.ANY)
    stays = pl.BlockSpec(memory_space=pltpu.HBM)
    out = pl.pallas_call(
        functools.partial(body, slabs, pools),
        out_shape=jax.ShapeDtypeStruct((slots, rows, length), f32),
        in_specs=[stays] * 7,
        out_specs=anywhere,
        scratch_shapes=[
            pltpu.SMEM(owner_table.shape, jnp.int32),
            pltpu.VMEM((slots, rows, length), f32),
            pltpu.VMEM((planes * length, length), f32),
            pltpu.VMEM(cutoff_mask.shape, jnp.int32),
            *[pltpu.VMEM(table.shape, bf16) for table in tables],
            pltpu.VMEM((planes * length, length), f32),
            *[pltpu.VMEM(field, f32)] * 3,
            *[pltpu.VMEM(cut, f32)] * 4,
            pltpu.VMEM(field, f32),
            pltpu.SemaphoreType.DMA((7,)),
            pltpu.SemaphoreType.DMA((owned,)),
            pltpu.SemaphoreType.DMA((3,)),
            pltpu.SemaphoreType.DMA((owned,)),
            pltpu.SemaphoreType.DMA((owned,)),
            pltpu.SemaphoreType.DMA((3,)),
        ],
        compiler_params=pltpu.CompilerParams(
            collective_id=0, has_side_effects=True, vmem_limit_bytes=44 * 2**20
        ),
        name="response",
    )(
        *[
            pltpu.with_memory_space_constraint(value, pltpu.HBM)
            for value in (
                owner_table,
                drho_part.reshape(slots, rows, length),
                fxc.reshape(planes * length, length),
                cutoff_mask,
                *[jnp.asarray(table) for table in tables],
            )
        ]
    )
    return out.reshape(slots, parts, planes, length, length)


def solution(mesh):
    placed = (
        P("pool", "group", None, "slab", None, None),
        P("slab", None, None),
        P(None, "slab", None),
        P("group"),
    )
    return jax.shard_map(
        functools.partial(per_device, mesh.shape["slab"], mesh.shape["pool"]),
        mesh=mesh,
        in_specs=placed,
        out_specs=P("group", None, "slab", None, None),
        check_vma=False,
    )
```

```python
import functools
import math

import jax
import jax.numpy as jnp
import numpy as np
from jax import lax
from jax.experimental import pallas as pl
from jax.experimental.pallas import tpu as pltpu
from jax.sharding import PartitionSpec as P

MESH = pl.DeviceIdType.MESH


def complex_form(table):
    return np.block([[table.real, -table.imag], [table.imag, table.real]])


def two_halves(table):
    high = table.astype(np.float32).astype(jnp.bfloat16)
    low = (table - high.astype(np.float64)).astype(np.float32).astype(jnp.bfloat16)
    return np.stack([high, low])


def dft_tables(length, width):
    tiles = length // width
    index = np.arange(length)
    phase = np.exp(-2j * math.pi * (index[:, None] * index[None, :] % length) / length)
    lanes = complex_form(phase).T
    real = complex_form(phase).reshape(2, length, 2, length)
    same = np.eye(width)
    cut = real.reshape(2, tiles, width, 2, length)
    spread = np.einsum("atibn,mk->tamibkn", cut, same)
    spread = spread.reshape(tiles * 2 * width * width, 2 * width * length)
    cut = real.reshape(2, length, 2, tiles, width)
    gather = np.einsum("anbtm,ik->aintbmk", cut, same)
    gather = gather.reshape(2 * width * length, tiles * 2 * width * width)
    return two_halves(lanes), two_halves(spread), two_halves(gather)


def split(value):
    high = value.astype(jnp.bfloat16)
    low = (value - high.astype(jnp.float32)).astype(jnp.bfloat16)
    return high, low


def from_left(table, value):
    high, low = split(value)
    lanes = value.shape[1]
    both = jnp.concatenate([high, low], axis=1)
    most = jnp.dot(table[0], both, preferred_element_type=jnp.float32)
    rest = jnp.dot(table[1], high, preferred_element_type=jnp.float32)
    return most[:, :lanes] + (most[:, lanes:] + rest)


def along_lanes(table, value):
    high, low = split(value)
    rows = value.shape[0]
    both = jnp.concatenate([high, low], axis=0)
    most = jnp.dot(both, table[0], preferred_element_type=jnp.float32)
    rest = jnp.dot(high, table[1], preferred_element_type=jnp.float32)
    return most[:rows] + (most[rows:] + rest)


def frequency(index, length):
    return ((index + length // 2) % length - length // 2).astype(jnp.float32)


def body(
    slabs, wide, pools, owner_hbm, drho_hbm, fxc_hbm, mask_hbm, lanes_hbm, spread_hbm, gather_hbm, out_hbm,
    owner_ref, drho, fxc, mask, lanes, spread, gather, kernel, other, given, density, sent, columns, back, final, result,
    load_sem, ready_sem, other_sem, send_sem, column_sem, final_sem, out_sem,
):
    me = lax.axis_index("slab")
    pool = lax.axis_index("pool")
    partner = pools - 1 - pool
    owned = given.shape[0]
    rows, length = given.shape[1:]
    half = rows // 2
    width = mask.shape[1]

    loads = [
        pltpu.make_async_copy(source, target, load_sem.at[n])
        for n, (source, target) in enumerate(
            [
                (owner_hbm, owner_ref),
                (drho_hbm, drho),
                (lanes_hbm, lanes),
                (spread_hbm, spread),
                (gather_hbm, gather),
                (mask_hbm, mask),
                (fxc_hbm, fxc),
            ]
        )
    ]
    for load in loads:
        load.start()

    barrier = pltpu.get_barrier_semaphore()
    turn = lax.rem(me + slabs - 1, slabs)
    row = turn // wide
    last = slabs // wide - 1

    def at(position):
        return lax.rem(position + 1, slabs)

    def tell(semaphore, to):
        pl.semaphore_signal(semaphore, inc=1, device_id={"slab": to}, device_id_type=MESH)

    def greet(to, _):
        @pl.when(to != turn)
        def _():
            tell(barrier, at(to))

        return 0

    lax.fori_loop(row * wide, slabs, greet, 0)
    pl.semaphore_signal(barrier, inc=1, device_id={"pool": partner}, device_id_type=MESH)
    pl.semaphore_wait(barrier, (row + 1) * wide)

    def announce(to, _):
        tell(ready_sem.at[row], at(to))
        return 0

    lax.fori_loop(0, row * wide, announce, 0)

    loads[0].wait()
    loads[1].wait()

    def pick(slot, _):
        other[slot] = drho[owner_ref[partner * owned + slot]]
        return 0

    lax.fori_loop(0, owned, pick, 0)

    def to_partner(slot):
        return pltpu.make_async_remote_copy(
            src_ref=other.at[slot],
            dst_ref=given.at[slot],
            send_sem=send_sem.at[0],
            recv_sem=other_sem.at[slot],
            device_id={"pool": partner},
            device_id_type=MESH,
        )

    def hand_over(slot, _):
        to_partner(slot).start()
        return 0

    lax.fori_loop(0, owned, hand_over, 0)

    def send(source, target, slot, to, arrived, left):
        pltpu.make_async_remote_copy(
            src_ref=source.at[slot, to],
            dst_ref=target.at[slot, me],
            send_sem=left,
            recv_sem=arrived.at[slot],
            device_id={"slab": to},
            device_id_type=MESH,
        ).start()

    def scatter(source, target, slot, among, arrived, left):
        def one(step, _):
            to = turn + step
            send(source, target, slot, at(jnp.where(to < among, to, to - among)), arrived, left)
            return 0

        lax.fori_loop(1, among, one, 0)
        target[slot, me] = source[slot, me]

    def scatter_down(source, target, slot, arrived, left):
        def one(step, _):
            to = lax.rem(me + slabs - step, slabs)
            send(source, target, slot, to, arrived, left)
            return 0

        lax.fori_loop(1, slabs, one, 0)
        target[slot, me] = source[slot, me]

    def await_all(target, slot, arrived):
        block = target.at[slot, pl.ds(0, slabs - 1)]
        pltpu.make_async_copy(block, block, arrived.at[slot]).wait()

    def await_sent(source, left):
        block = source.at[:, pl.ds(0, slabs - 1)]
        pltpu.make_async_copy(block, block, left).wait()

    loads[2].wait()
    loads[3].wait()

    def forward(slot):
        to_partner(slot).wait_recv()
        value = drho[owner_ref[pool * owned + slot]] + given[slot]
        density[slot] = value
        value = along_lanes(lanes, jnp.concatenate([value[:half], value[half:]], axis=1))
        value = from_left(spread, jnp.concatenate([value[:, :length], value[:, length:]], axis=0))
        sent[slot] = value.reshape(sent.shape[1:])

    early = 2
    for slot in range(early):
        forward(slot)
        scatter(sent, columns, slot, (row + 1) * wide, column_sem, send_sem.at[1])
    forward(early)

    def later_row(to_row, _):
        pl.semaphore_wait(ready_sem.at[to_row], wide)
        for slot in range(early):
            for step in range(wide):
                send(sent, columns, slot, at(to_row * wide + step), column_sem, send_sem.at[1])
        return 0

    lax.fori_loop(row + 1, last + 1, later_row, 0)

    def next_slot(slot, _):
        scatter(sent, columns, slot, slabs, column_sem, send_sem.at[1])

        @pl.when(slot + 1 < owned)
        def _():
            forward(slot + 1)

        return 0

    lax.fori_loop(early, owned, next_slot, 0)

    for load in loads[4:]:
        load.wait()
    unit = (2.0 * math.pi / length) ** 2
    shape = (length, length)
    first = frequency(lax.broadcasted_iota(jnp.int32, shape, 0), length) ** 2
    third = frequency(lax.broadcasted_iota(jnp.int32, shape, 1), length) ** 2
    for part in range(width):
        middle = frequency(jnp.full(shape, me * width + part, jnp.int32), length) ** 2
        total = first + middle + third
        kept = mask[:, part, :].astype(jnp.float32)
        kernel[pl.ds(part * length, length)] = (
            4.0 * math.pi * kept / (unit * total + 0.25) * (1.0 / length**3)
        )

    def screen(slot, _):
        await_all(columns, slot, column_sem)
        value = from_left(gather, columns[slot].reshape(rows, length))
        factor = kernel[...]
        value = jnp.concatenate([value[:half] * factor, value[half:] * -factor], axis=0)
        back[slot] = from_left(spread, value).reshape(back.shape[1:])
        scatter_down(back, final, slot, final_sem, send_sem.at[2])
        return 0

    lax.fori_loop(0, owned, screen, 0)

    def outgoing(slot):
        place = out_hbm.at[pool * owned + slot]
        keep = pltpu.make_async_copy(result.at[slot], place, out_sem.at[0])
        give = pltpu.make_async_remote_copy(
            src_ref=result.at[slot],
            dst_ref=place,
            send_sem=out_sem.at[1],
            recv_sem=out_sem.at[2],
            device_id={"pool": partner},
            device_id_type=MESH,
        )
        return keep, give

    def inverse(slot, _):
        await_all(final, slot, final_sem)
        value = from_left(gather, final[slot].reshape(rows, length))
        value = along_lanes(lanes, jnp.concatenate([value[:half], value[half:]], axis=1))
        local = fxc[...]
        result[slot, pl.ds(0, half)] = value[:, :length] + local * density[slot, pl.ds(0, half)]
        result[slot, pl.ds(half, half)] = local * density[slot, pl.ds(half, half)] - value[:, length:]
        keep, give = outgoing(slot)
        keep.start()
        give.start()
        return 0

    lax.fori_loop(0, owned, inverse, 0)

    pltpu.make_async_copy(other, other, send_sem.at[0]).wait()
    await_sent(sent, send_sem.at[1])
    await_sent(back, send_sem.at[2])
    for n in range(3):
        pltpu.make_async_copy(result, result, out_sem.at[n]).wait()


def per_device(slabs, pools, drho_part, fxc, cutoff_mask, owner_table):
    _, slots, parts, planes, length, _ = drho_part.shape
    rows = parts * planes * length
    owned = slots // pools
    wide = next(n for n in range(math.isqrt(slabs) // 2, 0, -1) if slabs % n == 0)
    tables = dft_tables(length, planes)
    tile = parts * planes * planes
    field = (owned, rows, length)
    cut = (owned, slabs, tile, length)
    bf16, f32 = jnp.bfloat16, jnp.float32
    anywhere = pl.BlockSpec(memory_space=pl.ANY)
    stays = pl.BlockSpec(memory_space=pltpu.HBM)
    out = pl.pallas_call(
        functools.partial(body, slabs, wide, pools),
        out_shape=jax.ShapeDtypeStruct((slots, rows, length), f32),
        in_specs=[stays] * 7,
        out_specs=anywhere,
        scratch_shapes=[
            pltpu.SMEM(owner_table.shape, jnp.int32),
            pltpu.VMEM((slots, rows, length), f32),
            pltpu.VMEM((planes * length, length), f32),
            pltpu.VMEM(cutoff_mask.shape, jnp.int32),
            *[pltpu.VMEM(table.shape, bf16) for table in tables],
            pltpu.VMEM((planes * length, length), f32),
            *[pltpu.VMEM(field, f32)] * 3,
            *[pltpu.VMEM(cut, f32)] * 4,
            pltpu.VMEM(field, f32),
            pltpu.SemaphoreType.DMA((7,)),
            pltpu.SemaphoreType.REGULAR((slabs // wide,)),
            pltpu.SemaphoreType.DMA((owned,)),
            pltpu.SemaphoreType.DMA((3,)),
            pltpu.SemaphoreType.DMA((owned,)),
            pltpu.SemaphoreType.DMA((owned,)),
            pltpu.SemaphoreType.DMA((3,)),
        ],
        compiler_params=pltpu.CompilerParams(
            collective_id=0, has_side_effects=True, vmem_limit_bytes=44 * 2**20
        ),
        name="response",
    )(
        *[
            pltpu.with_memory_space_constraint(value, pltpu.HBM)
            for value in (
                owner_table,
                drho_part.reshape(slots, rows, length),
                fxc.reshape(planes * length, length),
                cutoff_mask,
                *[jnp.asarray(table) for table in tables],
            )
        ]
    )
    return out.reshape(slots, parts, planes, length, length)


def solution(mesh):
    placed = (
        P("pool", "group", None, "slab", None, None),
        P("slab", None, None),
        P(None, "slab", None),
        P("group"),
    )
    return jax.shard_map(
        functools.partial(per_device, mesh.shape["slab"], mesh.shape["pool"]),
        mesh=mesh,
        in_specs=placed,
        out_specs=P("group", None, "slab", None, None),
        check_vma=False,
    )
```

```python
import functools
import math

import jax
import jax.numpy as jnp
import numpy as np
from jax import lax
from jax.experimental import pallas as pl
from jax.experimental.pallas import tpu as pltpu
from jax.sharding import PartitionSpec as P

MESH = pl.DeviceIdType.MESH


def complex_form(table):
    return np.block([[table.real, -table.imag], [table.imag, table.real]])


def two_halves(table):
    high = table.astype(np.float32).astype(jnp.bfloat16)
    low = (table - high.astype(np.float64)).astype(np.float32).astype(jnp.bfloat16)
    return np.stack([high, low])


def dft_tables(length, width):
    tiles = length // width
    index = np.arange(length)
    phase = np.exp(-2j * math.pi * (index[:, None] * index[None, :] % length) / length)
    lanes = complex_form(phase).T
    real = complex_form(phase).reshape(2, length, 2, length)
    same = np.eye(width)
    cut = real.reshape(2, tiles, width, 2, length)
    spread = np.einsum("atibn,mk->tamibkn", cut, same)
    spread = spread.reshape(tiles * 2 * width * width, 2 * width * length)
    cut = real.reshape(2, length, 2, tiles, width)
    gather = np.einsum("anbtm,ik->aintbmk", cut, same)
    gather = gather.reshape(2 * width * length, tiles * 2 * width * width)
    return two_halves(lanes), two_halves(spread), two_halves(gather)


def split(value):
    high = value.astype(jnp.bfloat16)
    low = (value - high.astype(jnp.float32)).astype(jnp.bfloat16)
    return high, low


def from_left(table, value):
    high, low = split(value)
    lanes = value.shape[1]
    both = jnp.concatenate([high, low], axis=1)
    most = jnp.dot(table[0], both, preferred_element_type=jnp.float32)
    rest = jnp.dot(table[1], high, preferred_element_type=jnp.float32)
    return most[:, :lanes] + (most[:, lanes:] + rest)


def along_lanes(table, value):
    high, low = split(value)
    rows = value.shape[0]
    both = jnp.concatenate([high, low], axis=0)
    most = jnp.dot(both, table[0], preferred_element_type=jnp.float32)
    rest = jnp.dot(high, table[1], preferred_element_type=jnp.float32)
    return most[:rows] + (most[rows:] + rest)


def frequency(index, length):
    return ((index + length // 2) % length - length // 2).astype(jnp.float32)


def body(
    slabs, wide, pools, owner_hbm, drho_hbm, fxc_hbm, mask_hbm, lanes_hbm, spread_hbm, gather_hbm, out_hbm,
    owner_ref, drho, fxc, mask, lanes, spread, gather, kernel, other, given, density, sent, columns, back, final, result,
    load_sem, ready_sem, other_sem, send_sem, column_sem, final_sem, out_sem,
):
    me = lax.axis_index("slab")
    pool = lax.axis_index("pool")
    partner = pools - 1 - pool
    owned = given.shape[0]
    rows, length = given.shape[1:]
    half = rows // 2
    width = mask.shape[1]

    loads = [
        pltpu.make_async_copy(source, target, load_sem.at[n])
        for n, (source, target) in enumerate(
            [
                (owner_hbm, owner_ref),
                (drho_hbm, drho),
                (lanes_hbm, lanes),
                (spread_hbm, spread),
                (gather_hbm, gather),
                (mask_hbm, mask),
                (fxc_hbm, fxc),
            ]
        )
    ]
    for load in loads:
        load.start()

    barrier = pltpu.get_barrier_semaphore()
    turn = lax.rem(me + slabs - 1, slabs)
    row = turn // wide
    last = slabs // wide - 1

    def at(position):
        return lax.rem(position + 1, slabs)

    def tell(semaphore, to):
        pl.semaphore_signal(semaphore, inc=1, device_id={"slab": to}, device_id_type=MESH)

    def greet(to, _):
        @pl.when(to != turn)
        def _():
            tell(barrier, at(to))

        return 0

    lax.fori_loop(row * wide, slabs, greet, 0)
    pl.semaphore_signal(barrier, inc=1, device_id={"pool": partner}, device_id_type=MESH)
    pl.semaphore_wait(barrier, (row + 1) * wide)

    def announce(to, _):
        tell(ready_sem.at[row], at(to))
        return 0

    lax.fori_loop(0, row * wide, announce, 0)

    loads[0].wait()
    loads[1].wait()

    def pick(slot, _):
        other[slot] = drho[owner_ref[partner * owned + slot]]
        return 0

    lax.fori_loop(0, owned, pick, 0)

    def to_partner(slot):
        return pltpu.make_async_remote_copy(
            src_ref=other.at[slot],
            dst_ref=given.at[slot],
            send_sem=send_sem.at[0],
            recv_sem=other_sem.at[slot],
            device_id={"pool": partner},
            device_id_type=MESH,
        )

    def hand_over(slot, _):
        to_partner(slot).start()
        return 0

    lax.fori_loop(0, owned, hand_over, 0)

    def send(source, target, slot, to, arrived, left):
        pltpu.make_async_remote_copy(
            src_ref=source.at[slot, to],
            dst_ref=target.at[slot, me],
            send_sem=left,
            recv_sem=arrived.at[slot],
            device_id={"slab": to},
            device_id_type=MESH,
        ).start()

    def scatter(source, target, slot, among, arrived, left):
        def one(step, _):
            to = turn + step
            send(source, target, slot, at(jnp.where(to < among, to, to - among)), arrived, left)
            return 0

        lax.fori_loop(1, among, one, 0)
        target[slot, me] = source[slot, me]

    def scatter_down(source, target, slot, arrived, left):
        def one(step, _):
            to = lax.rem(me + slabs - step, slabs)
            send(source, target, slot, to, arrived, left)
            return 0

        lax.fori_loop(1, slabs, one, 0)
        target[slot, me] = source[slot, me]

    def await_all(target, slot, arrived):
        block = target.at[slot, pl.ds(0, slabs - 1)]
        pltpu.make_async_copy(block, block, arrived.at[slot]).wait()

    def await_sent(source, left):
        block = source.at[:, pl.ds(0, slabs - 1)]
        pltpu.make_async_copy(block, block, left).wait()

    loads[2].wait()
    loads[3].wait()

    def forward(slot):
        to_partner(slot).wait_recv()
        value = drho[owner_ref[pool * owned + slot]] + given[slot]
        density[slot] = value
        value = along_lanes(lanes, jnp.concatenate([value[:half], value[half:]], axis=1))
        value = from_left(spread, jnp.concatenate([value[:, :length], value[:, length:]], axis=0))
        sent[slot] = value.reshape(sent.shape[1:])

    early = 2
    for slot in range(early):
        forward(slot)
        scatter(sent, columns, slot, (row + 1) * wide, column_sem, send_sem.at[1])
    forward(early)

    def later_row(to_row, _):
        pl.semaphore_wait(ready_sem.at[to_row], wide)
        for slot in range(early):
            for step in range(wide):
                send(sent, columns, slot, at(to_row * wide + step), column_sem, send_sem.at[1])
        return 0

    lax.fori_loop(row + 1, last + 1, later_row, 0)

    def next_slot(slot, _):
        scatter(sent, columns, slot, slabs, column_sem, send_sem.at[1])

        @pl.when(slot + 1 < owned)
        def _():
            forward(slot + 1)

        return 0

    lax.fori_loop(early, owned, next_slot, 0)

    for load in loads[4:]:
        load.wait()
    unit = (2.0 * math.pi / length) ** 2
    shape = (length, length)
    first = frequency(lax.broadcasted_iota(jnp.int32, shape, 0), length) ** 2
    third = frequency(lax.broadcasted_iota(jnp.int32, shape, 1), length) ** 2
    for part in range(width):
        middle = frequency(jnp.full(shape, me * width + part, jnp.int32), length) ** 2
        total = first + middle + third
        kept = mask[:, part, :].astype(jnp.float32)
        kernel[pl.ds(part * length, length)] = (
            4.0 * math.pi * kept / (unit * total + 0.25) * (1.0 / length**3)
        )

    def screen(slot, _):
        await_all(columns, slot, column_sem)
        value = from_left(gather, columns[slot].reshape(rows, length))
        factor = kernel[...]
        value = jnp.concatenate([value[:half] * factor, value[half:] * -factor], axis=0)
        back[slot] = from_left(spread, value).reshape(back.shape[1:])
        scatter_down(back, final, slot, final_sem, send_sem.at[2])
        return 0

    def outgoing(slot):
        place = out_hbm.at[pool * owned + slot]
        keep = pltpu.make_async_copy(result.at[slot], place, out_sem.at[0])
        give = pltpu.make_async_remote_copy(
            src_ref=result.at[slot],
            dst_ref=place,
            send_sem=out_sem.at[1],
            recv_sem=out_sem.at[2],
            device_id={"pool": partner},
            device_id_type=MESH,
        )
        return keep, give

    def inverse(slot, _):
        await_all(final, slot, final_sem)
        value = from_left(gather, final[slot].reshape(rows, length))
        value = along_lanes(lanes, jnp.concatenate([value[:half], value[half:]], axis=1))
        local = fxc[...]
        result[slot, pl.ds(0, half)] = value[:, :length] + local * density[slot, pl.ds(0, half)]
        result[slot, pl.ds(half, half)] = local * density[slot, pl.ds(half, half)] - value[:, length:]
        keep, give = outgoing(slot)
        keep.start()
        give.start()
        return 0

    lag = 2

    def both(slot, _):
        screen(slot, 0)
        return inverse(slot - lag, 0)

    lax.fori_loop(0, lag, screen, 0)
    lax.fori_loop(lag, owned, both, 0)
    lax.fori_loop(owned - lag, owned, inverse, 0)

    pltpu.make_async_copy(other, other, send_sem.at[0]).wait()
    await_sent(sent, send_sem.at[1])
    await_sent(back, send_sem.at[2])
    for n in range(3):
        pltpu.make_async_copy(result, result, out_sem.at[n]).wait()


def per_device(slabs, pools, drho_part, fxc, cutoff_mask, owner_table):
    _, slots, parts, planes, length, _ = drho_part.shape
    rows = parts * planes * length
    owned = slots // pools
    wide = next(n for n in range(math.isqrt(slabs) // 2, 0, -1) if slabs % n == 0)
    tables = dft_tables(length, planes)
    tile = parts * planes * planes
    field = (owned, rows, length)
    cut = (owned, slabs, tile, length)
    bf16, f32 = jnp.bfloat16, jnp.float32
    anywhere = pl.BlockSpec(memory_space=pl.ANY)
    stays = pl.BlockSpec(memory_space=pltpu.HBM)
    out = pl.pallas_call(
        functools.partial(body, slabs, wide, pools),
        out_shape=jax.ShapeDtypeStruct((slots, rows, length), f32),
        in_specs=[stays] * 7,
        out_specs=anywhere,
        scratch_shapes=[
            pltpu.SMEM(owner_table.shape, jnp.int32),
            pltpu.VMEM((slots, rows, length), f32),
            pltpu.VMEM((planes * length, length), f32),
            pltpu.VMEM(cutoff_mask.shape, jnp.int32),
            *[pltpu.VMEM(table.shape, bf16) for table in tables],
            pltpu.VMEM((planes * length, length), f32),
            *[pltpu.VMEM(field, f32)] * 3,
            *[pltpu.VMEM(cut, f32)] * 4,
            pltpu.VMEM(field, f32),
            pltpu.SemaphoreType.DMA((7,)),
            pltpu.SemaphoreType.REGULAR((slabs // wide,)),
            pltpu.SemaphoreType.DMA((owned,)),
            pltpu.SemaphoreType.DMA((3,)),
            pltpu.SemaphoreType.DMA((owned,)),
            pltpu.SemaphoreType.DMA((owned,)),
            pltpu.SemaphoreType.DMA((3,)),
        ],
        compiler_params=pltpu.CompilerParams(
            collective_id=0, has_side_effects=True, vmem_limit_bytes=44 * 2**20
        ),
        name="response",
    )(
        *[
            pltpu.with_memory_space_constraint(value, pltpu.HBM)
            for value in (
                owner_table,
                drho_part.reshape(slots, rows, length),
                fxc.reshape(planes * length, length),
                cutoff_mask,
                *[jnp.asarray(table) for table in tables],
            )
        ]
    )
    return out.reshape(slots, parts, planes, length, length)


def solution(mesh):
    placed = (
        P("pool", "group", None, "slab", None, None),
        P("slab", None, None),
        P(None, "slab", None),
        P("group"),
    )
    return jax.shard_map(
        functools.partial(per_device, mesh.shape["slab"], mesh.shape["pool"]),
        mesh=mesh,
        in_specs=placed,
        out_specs=P("group", None, "slab", None, None),
        check_vma=False,
    )
```
